32 devices in a mesh: image: 2 (over y), ga: 4 (over z), band: 4 (over x, core).
Axes of the slice: x: 2, y: 2, z: 4, core: 2. Of those that a mesh axis runs over, the one named last changes fastest.
Arguments:
- projectors: bfloat16 [160, 655360], P(('image', 'band'), 'ga'), parts along dimension 0, may hold values from -6 to 6
- occupied: bfloat16 [256, 655360], P(('image', 'band'), 'ga'), parts along dimension 0, may hold values from -0.0009765625 to 0.0009765625
- block: bfloat16 [512, 655360], P(('image', 'band'), 'ga'), parts along dimension 0, may hold values from -0.0078125 to 0.0078125
- weights: float32 [256], P(('image', 'band')), parts along dimension 0, may hold values from 0.1 to 1
- u_index: int32 [16], replicated, may hold values from 0 to 3
- u_values: float32 [4], replicated, may hold values from 0.5 to 2
Outputs:
- applied: bfloat16 [512, 655360], P(('image', 'band'), 'ga'), parts along dimension 0
The draws below stay inside these ranges and needn't reach their ends.
There are 2 independent parts, one for each index of `image`. The reference program is written for one: setup_inputs(seed, part) draws one part's arguments, and reference() takes and returns one part's arrays. A program takes and returns all parts, laid end to end along the dimension named above; an argument that names none is the same for every part. Nothing has to cross between parts.
Inputs may be any that keep to these rules, and one draw needn't show every extreme that they name: `u_index`: each atom's entry of the U table.
All inputs are finite; a program needn't handle non-finite values.
Results may differ from the reference program's by a relative error of at most 0.0049.
Values may be sent and summed in bfloat16 or wider, within the bound.
A program may use at most 192 MiB of HBM per device.

```python
import math
import jax
import jax.numpy as jnp
from jax import lax

NPW = 655360
ORB = 5
NAT = 16
NSPEC = 4
NOCC = 128
NBLK = 256
NPROJ = 80


def place_ends(drawn, key, low, top_value):
    longest = drawn.shape.index(max(drawn.shape))
    spots = []
    for shift in (0, 1):
        where = [jax.random.randint(jax.random.fold_in(key, axis), (), 0, length) for axis, length in enumerate(drawn.shape)]
        where[longest] = (where[longest] + shift) % drawn.shape[longest]
        spots.append(tuple(where))
    return drawn.at[spots[0]].set(low).at[spots[1]].set(top_value)


def levels(own_key, dims, shards, least, top_value):
    def one(position, parts):
        steps = jax.random.uniform(jax.random.fold_in(jax.random.fold_in(own_key, 6), position), (parts,), jnp.float32, least / len(shards), top_value / len(shards))
        return jnp.repeat(jnp.exp(steps), dims[position] // parts).reshape((-1,) + (1,) * (len(dims) - position - 1))

    gain = one(*shards[0])
    for cut in shards[1:]:
        gain = gain * one(*cut)
    return gain


def bell_draw(rng, dims, spread, most, pieces=(), kind=jnp.bfloat16):
    values = spread * jax.random.normal(rng, dims, jnp.float32)
    if pieces:
        values = values * levels(rng, dims, pieces, -0.22, 0.18)
    return jnp.clip(values, -most, most).astype(kind)


def setup_inputs(seed: int = 0, part: int = 0) -> dict:
    key_of = jax.random.split(jax.random.key(seed), 7)
    part_keys = jax.random.split(jax.random.fold_in(key_of[6], part), 7)
    return {
        "projectors": bell_draw(part_keys[0], (NPROJ, NPW), 1.0, 6.0, ((0, 4), (1, 4))),
        "occupied": bell_draw(part_keys[1], (NOCC, NPW), (NPW * NOCC // 2) ** -0.5, 0.0009765625, ((0, 4), (1, 4))),
        "block": bell_draw(part_keys[2], (NBLK, NPW), NPW ** -0.5, 0.0078125, ((0, 4), (1, 4))),
        "weights": jnp.clip(jnp.exp(math.log(1.0) - 2.3025851 * jax.random.uniform(part_keys[3], (NOCC,), jnp.float32) ** levels(part_keys[3], (NOCC,), ((0, 4),), -0.2, 0.2)), 0.1, 1.0),
        "u_index": place_ends(jax.random.randint(key_of[4], (NAT,), 0, NSPEC), jax.random.fold_in(key_of[4], 1), 0, NSPEC - 1).astype(jnp.int32),
        "u_values": jnp.clip(jnp.exp(jax.random.uniform(key_of[5], (NSPEC,), jnp.float32, math.log(0.5), math.log(2.0))), 0.5, 2.0),
    }


def reference(projectors, occupied, block, weights, u_index, u_values):
    proj_occ = jnp.dot(projectors, occupied.T, preferred_element_type=jnp.float32)
    proj_blk = jnp.dot(projectors, block.T, preferred_element_type=jnp.float32)
    shaped = proj_occ.reshape(NAT, ORB, NOCC)
    occ = jnp.einsum("amb,anb->amn", shaped * weights[None, None, :], shaped, precision=lax.Precision.HIGHEST)
    selector = (u_index[:, None] == jnp.arange(NSPEC, dtype=jnp.int32)[None, :]).astype(jnp.float32)
    u_atom = jnp.dot(selector, u_values, precision=lax.Precision.HIGHEST)
    potential = u_atom[:, None, None] * (0.5 * jnp.eye(ORB, dtype=jnp.float32)[None] - occ)
    hub_coef = jnp.einsum("amn,anc->amc", potential, proj_blk.reshape(NAT, ORB, NBLK), precision=lax.Precision.HIGHEST)
    hub_coef = hub_coef.reshape(NPROJ, NBLK).astype(jnp.bfloat16)
    applied = jnp.dot(hub_coef.T, projectors, preferred_element_type=jnp.float32)
    return applied.astype(jnp.bfloat16)
```

```python
import functools
import math

import jax
import jax.numpy as jnp
from jax import lax
from jax.experimental import pallas as pl
from jax.experimental.pallas import tpu as pltpu
from jax.sharding import PartitionSpec as P

ORB = 5
LANES = 128
SUBLANES = 8
CORES = 2
STEPS = 16
SMALL = 5
BLOCKS = 40
DEEP = 4
MESH = pl.DeviceIdType.MESH
NT = (((1,), (1,)), ((), ()))


def most_steps(columns, limit):
    units = columns // LANES
    return max(s for s in range(1, limit + 1) if units % s == 0)


def round_up(n, to):
    return -(-n // to) * to


def plan(part):
    steps = most_steps(part, STEPS)
    width = part // steps
    tail, left = [], width // LANES
    while left > SMALL:
        tail.append(left - left // 2)
        left //= 2
    tail.append(left)
    tail = [t * LANES for t in tail]
    starts = [(steps - 1) * width + sum(tail[:i]) for i in range(len(tail))]
    return steps - 1, width, list(zip(starts, tail))


def gather_kernel(
    shards, groups, folds,
    p_ref, occ_ref, blk_ref, weights_ref, index_ref, table_ref,
    all_ref, hub_ref,
    raw, bands, acc, proj, proj_all, diag, diag_all, select, scale, weight,
    raw_sem, band_sem, chip_send, core_send, recv, ga_send, ga_recv, sum_send, sum_recv,
):
    chips = shards // CORES
    rows, columns = p_ref.shape
    part = columns // folds
    packed = rows * folds
    main, width, tail = plan(part)
    count = main + len(tail)
    n_occ, n_blk = occ_ref.shape[0], blk_ref.shape[0]
    both = n_occ + n_blk
    total = shards * rows
    wide = bands.shape[2]
    lanes = proj.shape[1]
    me = lax.axis_index("band")
    chip, core = me // CORES, lax.rem(me, CORES)
    ga = lax.axis_index("ga")
    partner = chip * CORES + (1 - core)

    def band_at(distance):
        return lax.rem(chip + distance, chips) * CORES + core

    def span(step):
        if isinstance(step, int) and step >= main:
            return tail[step - main]
        return pl.multiple_of(step * width, LANES), width

    def raw_copy(step, fold):
        start, w = span(step)
        return pltpu.make_async_copy(
            p_ref.at[:, pl.ds(fold * part + start, w)],
            raw.at[fold, :, pl.ds(start, w)],
            raw_sem.at[step, fold],
        )

    def band_copies(step):
        start, w = span(step)
        slot = lax.rem(step, 2)
        found = []
        for fold in range(folds):
            cols = pl.ds(fold * part + start, w)
            found.append(pltpu.make_async_copy(
                occ_ref.at[:, cols], bands.at[slot, fold, pl.ds(0, n_occ), pl.ds(0, w)], band_sem.at[slot, fold, 0]))
            found.append(pltpu.make_async_copy(
                blk_ref.at[:, cols], bands.at[slot, fold, pl.ds(n_occ, n_blk), pl.ds(0, w)], band_sem.at[slot, fold, 1]))
        return found

    def rows_of(step, owner):
        start, w = span(step)
        return all_ref.at[pl.ds(pl.multiple_of(owner * packed, SUBLANES), packed), pl.ds(start, w)]

    def to_chip(step, distance):
        slot = CORES * ((chips - distance) % chips)
        return pltpu.make_async_remote_copy(
            src_ref=rows_of(step, me), dst_ref=rows_of(step, me),
            send_sem=chip_send.at[step, distance], recv_sem=recv.at[step, slot],
            device_id={"band": band_at(distance)}, device_id_type=MESH)

    def to_core(step, distance):
        return pltpu.make_async_remote_copy(
            src_ref=rows_of(step, band_at(distance)), dst_ref=rows_of(step, band_at(distance)),
            send_sem=core_send.at[step, distance], recv_sem=recv.at[step, CORES * distance + 1],
            device_id={"band": partner}, device_id_type=MESH)

    def pack(step):
        start, w = span(step)
        for fold in range(folds):
            raw_copy(step, fold).wait()
        pieces = [raw[fold, :, pl.ds(start, w)].astype(jnp.float32) for fold in range(folds)]
        all_ref[pl.ds(pl.multiple_of(me * packed, SUBLANES), packed), pl.ds(start, w)] = (
            jnp.concatenate(pieces, axis=0).astype(all_ref.dtype))

    def send(step):
        for distance in range(1, chips):
            to_chip(step, distance).start()
        to_core(step, 0).start()

    for fold in range(folds):
        raw_copy(0, fold).start()
    barrier = pltpu.get_barrier_semaphore()
    for k in range(1, shards):
        pl.semaphore_signal(barrier, inc=1, device_id={"band": lax.rem(me + k, shards)}, device_id_type=MESH)
    for k in range(1, groups):
        pl.semaphore_signal(barrier, inc=1, device_id={"ga": lax.rem(ga + k, groups)}, device_id_type=MESH)
    pack(0)
    pl.semaphore_wait(barrier, shards + groups - 2)
    send(0)

    def fetch(step):
        for fold in range(folds):
            raw_copy(step, fold).start()

    def loop(first, last, body):
        def run(step, carry):
            body(step)
            return carry
        lax.fori_loop(first, last, run, 0)

    loop(1, main, fetch)
    for step in range(max(main, 1), count):
        fetch(step)
    for copy in band_copies(0):
        copy.start()

    def pack_send(step):
        pack(step)
        send(step)

    loop(1, main, pack_send)
    for step in range(max(main, 1), count):
        pack_send(step)

    acc[...] = jnp.zeros_like(acc)
    if wide > both:
        for slot in range(2):
            for fold in range(folds):
                bands[slot, fold, pl.ds(both, wide - both)] = jnp.zeros((wide - both, width), bands.dtype)
    shape = (lanes, shards * packed)
    row = lax.broadcasted_iota(jnp.int32, shape, 0)
    col = lax.broadcasted_iota(jnp.int32, shape, 1)
    for fold in range(folds):
        hits = jnp.zeros(shape, jnp.float32)
        for owner in range(shards):
            low = owner * packed + fold * rows
            hit = (col >= low) & (col < low + rows) & (col - row == low - owner * rows)
            hits = hits + jnp.where(hit, 1.0, 0.0)
        select[fold] = hits.astype(select.dtype)
    lane = lax.broadcasted_iota(jnp.int32, (SUBLANES, lanes), 1)
    values = jnp.zeros((SUBLANES, lanes), jnp.float32)
    orbital = jnp.zeros((SUBLANES, lanes), jnp.int32)
    for atom in range(total // ORB):
        inside = (lane >= atom * ORB) & (lane < (atom + 1) * ORB)
        values = jnp.where(inside, table_ref[index_ref[atom]], values)
        orbital = jnp.where(inside, lane - atom * ORB, orbital)
    scale[...] = values
    one = lax.broadcasted_iota(jnp.int32, (n_occ, n_occ), 0)
    two = lax.broadcasted_iota(jnp.int32, (n_occ, n_occ), 1)
    column = jnp.sum(jnp.where(one == two, jnp.broadcast_to(weights_ref[...], (n_occ, n_occ)), 0.0), axis=1, keepdims=True)
    weight[...] = jnp.broadcast_to(column, weight.shape)

    def use(step):
        start, w = span(step)
        slot = lax.rem(step, 2)
        for distance in range(1, chips):
            to_chip(step, chips - distance).wait_recv()
            to_core(step, distance).start()
        for copy in band_copies(step):
            copy.wait()
        for distance in range(chips):
            to_core(step, distance).wait_recv()
        held = all_ref[:, pl.ds(start, w)]
        for fold in range(folds):
            acc[fold] += lax.dot_general(
                held, bands[slot, fold, :, pl.ds(0, w)], NT, preferred_element_type=jnp.float32)

    def sent(step):
        for distance in range(1, chips):
            to_chip(step, distance).wait_send()
        for distance in range(chips):
            to_core(step, distance).wait_send()

    def use_main(step):
        for copy in band_copies(step + 1):
            copy.start()
        use(step)
        sent(step)

    loop(0, main - 1, use_main)
    for step in range(max(main - 1, 0), count):
        if step + 1 < count:
            for copy in band_copies(step + 1):
                copy.start()
        use(step)

    pieces = []
    for owner in range(shards):
        piece = acc[0, pl.ds(owner * packed, rows)]
        for fold in range(1, folds):
            piece = piece + acc[fold, pl.ds(owner * packed + fold * rows, rows)]
        pieces.append(piece)
    if lanes > total:
        pieces.append(jnp.zeros((lanes - total, wide), jnp.float32))
    own = jnp.transpose(jnp.concatenate(pieces, axis=0))
    proj[...] = own

    def to_group(k, part_of):
        low, size = ((0, n_occ), (n_occ, n_blk))[part_of]
        return pltpu.make_async_remote_copy(
            src_ref=proj.at[pl.ds(low, size)], dst_ref=proj_all.at[k, pl.ds(low, size)],
            send_sem=ga_send.at[k, part_of], recv_sem=ga_recv.at[k, part_of],
            device_id={"ga": lax.rem(ga + k, groups)}, device_id_type=MESH)

    for part_of in range(2):
        for k in range(1, groups):
            to_group(k, part_of).start()
    for step in range(max(main - 1, 0), count):
        sent(step)
    mine = own[:n_occ]
    for k in range(1, groups):
        to_group(k, 0).wait_recv()
        mine = mine + proj_all[k, pl.ds(0, n_occ)]
    weighted = mine * weight[...]
    found = []
    for gap in range(ORB):
        moved = mine if gap == 0 else pltpu.roll(mine, lanes - gap, 1)
        found.append(jnp.sum(weighted * moved, axis=0, keepdims=True))
    found.append(jnp.zeros((SUBLANES - ORB, lanes), jnp.float32))
    occ = jnp.concatenate(found, axis=0)
    diag[...] = occ

    def to_band(k):
        return pltpu.make_async_remote_copy(
            src_ref=diag, dst_ref=diag_all.at[k], send_sem=sum_send.at[k], recv_sem=sum_recv.at[k],
            device_id={"band": lax.rem(me + k, shards)}, device_id_type=MESH)

    for k in range(1, shards):
        to_band(k).start()
    block = own[n_occ:both]
    for k in range(1, groups):
        to_group(k, 1).wait_recv()
        block = block + proj_all[k, pl.ds(n_occ, n_blk)]
    for k in range(1, shards):
        to_band(k).wait_recv()
        occ = occ + diag_all[k]
    u = scale[pl.ds(0, 1)]
    m = orbital[0:1]
    hub = (u * (0.5 - occ[0:1])) * block
    for gap in range(1, ORB):
        pair = -occ[gap:gap + 1]
        above = jnp.where(m + gap < ORB, u * pair, 0.0)
        below = jnp.where(m - gap >= 0, u * pltpu.roll(pair, gap, 1), 0.0)
        hub = hub + above * pltpu.roll(block, lanes - gap, 1) + below * pltpu.roll(block, gap, 1)
    hub = hub.astype(jnp.bfloat16)
    for fold in range(folds):
        hub_ref[pl.ds(fold * n_blk, n_blk)] = jnp.dot(
            hub, select[fold], preferred_element_type=jnp.float32).astype(jnp.bfloat16)

    for k in range(1, groups):
        for part_of in range(2):
            to_group(k, part_of).wait_send()
    for k in range(1, shards):
        to_band(k).wait_send()


def apply_kernel(folds, blocks, hub_ref, all_ref, out_ref, done, sems):
    bands = out_ref.shape[0]
    part = out_ref.shape[1] // folds
    tile = part // blocks
    deep = done.shape[0]

    def stores(step):
        slot = lax.rem(step, deep)
        start = pl.multiple_of(step * tile, LANES)
        return [pltpu.make_async_copy(
            done.at[slot, pl.ds(fold * bands, bands)],
            out_ref.at[:, pl.ds(fold * part + start, tile)],
            sems.at[slot, fold],
        ) for fold in range(folds)]

    def run(step, carry):
        @pl.when(step >= deep)
        def _():
            for copy in stores(step - deep):
                copy.wait()

        done[lax.rem(step, deep)] = jnp.dot(
            hub_ref[...], all_ref[:, pl.ds(pl.multiple_of(step * tile, LANES), tile)],
            preferred_element_type=jnp.float32).astype(done.dtype)
        for copy in stores(step):
            copy.start()
        return carry

    lax.fori_loop(0, blocks, run, 0)
    for step in range(max(blocks - deep, 0), blocks):
        for copy in stores(step):
            copy.wait()


def per_device(shards, groups, projectors, occupied, block, weights, u_index, u_values):
    rows, columns = projectors.shape
    n_occ, n_blk = occupied.shape[0], block.shape[0]
    folds = SUBLANES // math.gcd(rows, SUBLANES)
    part = columns // folds
    main, width, tail = plan(part)
    count = main + len(tail)
    packed, total = rows * folds, rows * shards
    wide = round_up(n_occ + n_blk, LANES)
    lanes = round_up(total, LANES)
    anywhere = pl.BlockSpec(memory_space=pl.ANY)
    scalars = pl.BlockSpec(memory_space=pltpu.SMEM)
    vector = pl.BlockSpec(memory_space=pltpu.VMEM)
    dma = pltpu.SemaphoreType.DMA
    chips = shards // CORES
    gathered, hub = pl.pallas_call(
        functools.partial(gather_kernel, shards, groups, folds),
        out_shape=(
            pltpu.VMEM((shards * packed, part), projectors.dtype),
            pltpu.VMEM((folds * n_blk, shards * packed), jnp.bfloat16),
        ),
        in_specs=[anywhere, anywhere, anywhere, vector, scalars, scalars],
        out_specs=(vector, vector),
        scratch_shapes=[
            pltpu.VMEM((folds, rows, part), projectors.dtype),
            pltpu.VMEM((2, folds, wide, width), occupied.dtype),
            pltpu.VMEM((folds, shards * packed, wide), jnp.float32),
            pltpu.VMEM((wide, lanes), jnp.float32),
            pltpu.VMEM((groups, wide, lanes), jnp.float32),
            pltpu.VMEM((SUBLANES, lanes), jnp.float32),
            pltpu.VMEM((shards, SUBLANES, lanes), jnp.float32),
            pltpu.VMEM((folds, lanes, shards * packed), jnp.bfloat16),
            pltpu.VMEM((SUBLANES, lanes), jnp.float32),
            pltpu.VMEM((n_occ, lanes), jnp.float32),
            dma((count, folds)),
            dma((2, folds, 2)),
            dma((count, chips)),
            dma((count, chips)),
            dma((count, shards)),
            dma((groups, 2)),
            dma((groups, 2)),
            dma((shards,)),
            dma((shards,)),
        ],
        compiler_params=pltpu.CompilerParams(
            collective_id=0, has_side_effects=True, vmem_limit_bytes=24 * 2**20
        ),
        name="gather_project",
    )(projectors, occupied, block, weights.reshape(1, n_occ), u_index, u_values)

    blocks = most_steps(part, BLOCKS)
    tile = part // blocks
    deep = min(DEEP, blocks)
    return pl.pallas_call(
        functools.partial(apply_kernel, folds, blocks),
        out_shape=jax.ShapeDtypeStruct((n_blk, columns), block.dtype),
        in_specs=[vector, vector],
        out_specs=anywhere,
        scratch_shapes=[
            pltpu.VMEM((deep, folds * n_blk, tile), block.dtype),
            dma((deep, folds)),
        ],
        compiler_params=pltpu.CompilerParams(vmem_limit_bytes=24 * 2**20),
        name="apply_potential",
    )(hub, gathered)


def solution(mesh):
    spread = P(("image", "band"), "ga")
    in_specs = (spread, spread, spread, P(("image", "band")), P(), P())
    return jax.shard_map(
        functools.partial(per_device, mesh.shape["band"], mesh.shape["ga"]),
        mesh=mesh, in_specs=in_specs, out_specs=spread, check_vma=False,
    )
```

```python
import functools
import math

import jax
import jax.numpy as jnp
from jax import lax
from jax.experimental import pallas as pl
from jax.experimental.pallas import tpu as pltpu
from jax.sharding import PartitionSpec as P

ORB = 5
LANES = 128
SUBLANES = 8
CORES = 2
STEPS = 16
SMALL = 5
BLOCKS = 40
DEEP = 4
MESH = pl.DeviceIdType.MESH
NT = (((1,), (1,)), ((), ()))


def most_steps(columns, limit):
    units = columns // LANES
    return max(s for s in range(1, limit + 1) if units % s == 0)


def round_up(n, to):
    return -(-n // to) * to


def plan(part):
    steps = most_steps(part, STEPS)
    width = part // steps
    tail, left = [], width // LANES
    while left > SMALL:
        tail.append(left - left // 2)
        left //= 2
    tail.append(left)
    tail = [t * LANES for t in tail]
    starts = [(steps - 1) * width + sum(tail[:i]) for i in range(len(tail))]
    return steps - 1, width, list(zip(starts, tail))


def gather_kernel(
    shards, groups, folds,
    p_ref, occ_ref, blk_ref, weights_hbm, index_hbm, table_hbm,
    all_ref, hub_ref,
    weights_ref, index_ref, table_ref, raw, bands, acc, proj, proj_all, diag, diag_all, select, scale, weight,
    small_sem, raw_sem, band_sem, chip_send, core_send, recv, ga_send, ga_recv, sum_send, sum_recv,
):
    chips = shards // CORES
    rows, columns = p_ref.shape
    part = columns // folds
    packed = rows * folds
    main, width, tail = plan(part)
    count = main + len(tail)
    n_occ, n_blk = occ_ref.shape[0], blk_ref.shape[0]
    both = n_occ + n_blk
    total = shards * rows
    wide = bands.shape[2]
    lanes = proj.shape[1]
    me = lax.axis_index("band")
    chip, core = me // CORES, lax.rem(me, CORES)
    ga = lax.axis_index("ga")
    partner = chip * CORES + (1 - core)

    def band_at(distance):
        return lax.rem(chip + distance, chips) * CORES + core

    def span(step):
        if isinstance(step, int) and step >= main:
            return tail[step - main]
        return pl.multiple_of(step * width, LANES), width

    def raw_copy(step, fold):
        start, w = span(step)
        return pltpu.make_async_copy(
            p_ref.at[:, pl.ds(fold * part + start, w)],
            raw.at[fold, :, pl.ds(start, w)],
            raw_sem.at[step, fold],
        )

    def band_copies(step):
        start, w = span(step)
        slot = lax.rem(step, 2)
        found = []
        for fold in range(folds):
            cols = pl.ds(fold * part + start, w)
            found.append(pltpu.make_async_copy(
                occ_ref.at[:, cols], bands.at[slot, fold, pl.ds(0, n_occ), pl.ds(0, w)], band_sem.at[slot, fold, 0]))
            found.append(pltpu.make_async_copy(
                blk_ref.at[:, cols], bands.at[slot, fold, pl.ds(n_occ, n_blk), pl.ds(0, w)], band_sem.at[slot, fold, 1]))
        return found

    def rows_of(step, owner):
        start, w = span(step)
        return all_ref.at[pl.ds(pl.multiple_of(owner * packed, SUBLANES), packed), pl.ds(start, w)]

    def to_chip(step, distance):
        slot = CORES * ((chips - distance) % chips)
        return pltpu.make_async_remote_copy(
            src_ref=rows_of(step, me), dst_ref=rows_of(step, me),
            send_sem=chip_send.at[step, distance], recv_sem=recv.at[step, slot],
            device_id={"band": band_at(distance)}, device_id_type=MESH)

    def to_core(step, distance):
        return pltpu.make_async_remote_copy(
            src_ref=rows_of(step, band_at(distance)), dst_ref=rows_of(step, band_at(distance)),
            send_sem=core_send.at[step, distance], recv_sem=recv.at[step, CORES * distance + 1],
            device_id={"band": partner}, device_id_type=MESH)

    def pack(step):
        start, w = span(step)
        for fold in range(folds):
            raw_copy(step, fold).wait()
        pieces = [raw[fold, :, pl.ds(start, w)].astype(jnp.float32) for fold in range(folds)]
        all_ref[pl.ds(pl.multiple_of(me * packed, SUBLANES), packed), pl.ds(start, w)] = (
            jnp.concatenate(pieces, axis=0).astype(all_ref.dtype))

    def send(step):
        for distance in range(1, chips):
            to_chip(step, distance).start()
        to_core(step, 0).start()

    for fold in range(folds):
        raw_copy(0, fold).start()
    barrier = pltpu.get_barrier_semaphore()
    for k in range(1, shards):
        pl.semaphore_signal(barrier, inc=1, device_id={"band": lax.rem(me + k, shards)}, device_id_type=MESH)
    for k in range(1, groups):
        pl.semaphore_signal(barrier, inc=1, device_id={"ga": lax.rem(ga + k, groups)}, device_id_type=MESH)
    pack(0)
    pl.semaphore_wait(barrier, shards + groups - 2)
    send(0)

    small = [
        pltpu.make_async_copy(source, target, small_sem.at[k])
        for k, (source, target) in enumerate(
            ((weights_hbm, weights_ref), (index_hbm, index_ref), (table_hbm, table_ref)))
    ]
    for copy in small:
        copy.start()

    def fetch(step):
        for fold in range(folds):
            raw_copy(step, fold).start()

    def loop(first, last, body):
        def run(step, carry):
            body(step)
            return carry
        lax.fori_loop(first, last, run, 0)

    loop(1, main, fetch)
    for step in range(max(main, 1), count):
        fetch(step)
    for copy in band_copies(0):
        copy.start()

    def pack_send(step):
        pack(step)
        send(step)

    loop(1, main, pack_send)
    for step in range(max(main, 1), count):
        pack_send(step)

    acc[...] = jnp.zeros_like(acc)
    if wide > both:
        for slot in range(2):
            for fold in range(folds):
                bands[slot, fold, pl.ds(both, wide - both)] = jnp.zeros((wide - both, width), bands.dtype)
    shape = (lanes, shards * packed)
    row = lax.broadcasted_iota(jnp.int32, shape, 0)
    col = lax.broadcasted_iota(jnp.int32, shape, 1)
    for fold in range(folds):
        hits = jnp.zeros(shape, jnp.float32)
        for owner in range(shards):
            low = owner * packed + fold * rows
            hit = (col >= low) & (col < low + rows) & (col - row == low - owner * rows)
            hits = hits + jnp.where(hit, 1.0, 0.0)
        select[fold] = hits.astype(select.dtype)
    for copy in small:
        copy.wait()
    lane = lax.broadcasted_iota(jnp.int32, (SUBLANES, lanes), 1)
    values = jnp.zeros((SUBLANES, lanes), jnp.float32)
    orbital = jnp.zeros((SUBLANES, lanes), jnp.int32)
    for atom in range(total // ORB):
        inside = (lane >= atom * ORB) & (lane < (atom + 1) * ORB)
        values = jnp.where(inside, table_ref[index_ref[atom]], values)
        orbital = jnp.where(inside, lane - atom * ORB, orbital)
    scale[...] = values
    one = lax.broadcasted_iota(jnp.int32, (n_occ, n_occ), 0)
    two = lax.broadcasted_iota(jnp.int32, (n_occ, n_occ), 1)
    column = jnp.sum(jnp.where(one == two, jnp.broadcast_to(weights_ref[...], (n_occ, n_occ)), 0.0), axis=1, keepdims=True)
    weight[...] = jnp.broadcast_to(column, weight.shape)

    def use(step):
        start, w = span(step)
        slot = lax.rem(step, 2)
        for distance in range(1, chips):
            to_chip(step, chips - distance).wait_recv()
            to_core(step, distance).start()
        for copy in band_copies(step):
            copy.wait()
        for distance in range(chips):
            to_core(step, distance).wait_recv()
        held = all_ref[:, pl.ds(start, w)]
        for fold in range(folds):
            acc[fold] += lax.dot_general(
                held, bands[slot, fold, :, pl.ds(0, w)], NT, preferred_element_type=jnp.float32)

    def sent(step):
        for distance in range(1, chips):
            to_chip(step, distance).wait_send()
        for distance in range(chips):
            to_core(step, distance).wait_send()

    def use_main(step):
        for copy in band_copies(step + 1):
            copy.start()
        use(step)
        sent(step)

    loop(0, main - 1, use_main)
    for step in range(max(main - 1, 0), count):
        if step + 1 < count:
            for copy in band_copies(step + 1):
                copy.start()
        use(step)

    pieces = []
    for owner in range(shards):
        piece = acc[0, pl.ds(owner * packed, rows)]
        for fold in range(1, folds):
            piece = piece + acc[fold, pl.ds(owner * packed + fold * rows, rows)]
        pieces.append(piece)
    if lanes > total:
        pieces.append(jnp.zeros((lanes - total, wide), jnp.float32))
    own = jnp.transpose(jnp.concatenate(pieces, axis=0))
    proj[...] = own

    def to_group(k, part_of):
        low, size = ((0, n_occ), (n_occ, n_blk))[part_of]
        return pltpu.make_async_remote_copy(
            src_ref=proj.at[pl.ds(low, size)], dst_ref=proj_all.at[k, pl.ds(low, size)],
            send_sem=ga_send.at[k, part_of], recv_sem=ga_recv.at[k, part_of],
            device_id={"ga": lax.rem(ga + k, groups)}, device_id_type=MESH)

    for part_of in range(2):
        for k in range(1, groups):
            to_group(k, part_of).start()
    for step in range(max(main - 1, 0), count):
        sent(step)
    mine = own[:n_occ]
    for k in range(1, groups):
        to_group(k, 0).wait_recv()
        mine = mine + proj_all[k, pl.ds(0, n_occ)]
    weighted = mine * weight[...]
    found = []
    for gap in range(ORB):
        moved = mine if gap == 0 else pltpu.roll(mine, lanes - gap, 1)
        found.append(jnp.sum(weighted * moved, axis=0, keepdims=True))
    found.append(jnp.zeros((SUBLANES - ORB, lanes), jnp.float32))
    occ = jnp.concatenate(found, axis=0)
    diag[...] = occ

    def to_band(k):
        return pltpu.make_async_remote_copy(
            src_ref=diag, dst_ref=diag_all.at[k], send_sem=sum_send.at[k], recv_sem=sum_recv.at[k],
            device_id={"band": lax.rem(me + k, shards)}, device_id_type=MESH)

    for k in range(1, shards):
        to_band(k).start()
    block = own[n_occ:both]
    for k in range(1, groups):
        to_group(k, 1).wait_recv()
        block = block + proj_all[k, pl.ds(n_occ, n_blk)]
    for k in range(1, shards):
        to_band(k).wait_recv()
        occ = occ + diag_all[k]
    u = scale[pl.ds(0, 1)]
    m = orbital[0:1]
    hub = (u * (0.5 - occ[0:1])) * block
    for gap in range(1, ORB):
        pair = -occ[gap:gap + 1]
        above = jnp.where(m + gap < ORB, u * pair, 0.0)
        below = jnp.where(m - gap >= 0, u * pltpu.roll(pair, gap, 1), 0.0)
        hub = hub + above * pltpu.roll(block, lanes - gap, 1) + below * pltpu.roll(block, gap, 1)
    hub = hub.astype(jnp.bfloat16)
    for fold in range(folds):
        hub_ref[pl.ds(fold * n_blk, n_blk)] = jnp.dot(
            hub, select[fold], preferred_element_type=jnp.float32).astype(jnp.bfloat16)

    for k in range(1, groups):
        for part_of in range(2):
            to_group(k, part_of).wait_send()
    for k in range(1, shards):
        to_band(k).wait_send()


def apply_kernel(folds, blocks, hub_ref, all_ref, out_ref, done, sems):
    bands = out_ref.shape[0]
    part = out_ref.shape[1] // folds
    tile = part // blocks
    deep = done.shape[0]

    def stores(step):
        slot = lax.rem(step, deep)
        start = pl.multiple_of(step * tile, LANES)
        return [pltpu.make_async_copy(
            done.at[slot, pl.ds(fold * bands, bands)],
            out_ref.at[:, pl.ds(fold * part + start, tile)],
            sems.at[slot, fold],
        ) for fold in range(folds)]

    def run(step, carry):
        @pl.when(step >= deep)
        def _():
            for copy in stores(step - deep):
                copy.wait()

        done[lax.rem(step, deep)] = jnp.dot(
            hub_ref[...], all_ref[:, pl.ds(pl.multiple_of(step * tile, LANES), tile)],
            preferred_element_type=jnp.float32).astype(done.dtype)
        for copy in stores(step):
            copy.start()
        return carry

    lax.fori_loop(0, blocks, run, 0)
    for step in range(max(blocks - deep, 0), blocks):
        for copy in stores(step):
            copy.wait()


def per_device(shards, groups, projectors, occupied, block, weights, u_index, u_values):
    rows, columns = projectors.shape
    n_occ, n_blk = occupied.shape[0], block.shape[0]
    folds = SUBLANES // math.gcd(rows, SUBLANES)
    part = columns // folds
    main, width, tail = plan(part)
    count = main + len(tail)
    packed, total = rows * folds, rows * shards
    wide = round_up(n_occ + n_blk, LANES)
    lanes = round_up(total, LANES)
    anywhere = pl.BlockSpec(memory_space=pl.ANY)
    vector = pl.BlockSpec(memory_space=pltpu.VMEM)
    dma = pltpu.SemaphoreType.DMA
    chips = shards // CORES
    gathered, hub = pl.pallas_call(
        functools.partial(gather_kernel, shards, groups, folds),
        out_shape=(
            pltpu.VMEM((shards * packed, part), projectors.dtype),
            pltpu.VMEM((folds * n_blk, shards * packed), jnp.bfloat16),
        ),
        in_specs=[anywhere] * 6,
        out_specs=(vector, vector),
        scratch_shapes=[
            pltpu.VMEM((1, n_occ), jnp.float32),
            pltpu.SMEM(u_index.shape, u_index.dtype),
            pltpu.SMEM(u_values.shape, u_values.dtype),
            pltpu.VMEM((folds, rows, part), projectors.dtype),
            pltpu.VMEM((2, folds, wide, width), occupied.dtype),
            pltpu.VMEM((folds, shards * packed, wide), jnp.float32),
            pltpu.VMEM((wide, lanes), jnp.float32),
            pltpu.VMEM((groups, wide, lanes), jnp.float32),
            pltpu.VMEM((SUBLANES, lanes), jnp.float32),
            pltpu.VMEM((shards, SUBLANES, lanes), jnp.float32),
            pltpu.VMEM((folds, lanes, shards * packed), jnp.bfloat16),
            pltpu.VMEM((SUBLANES, lanes), jnp.float32),
            pltpu.VMEM((n_occ, lanes), jnp.float32),
            dma((3,)),
            dma((count, folds)),
            dma((2, folds, 2)),
            dma((count, chips)),
            dma((count, chips)),
            dma((count, shards)),
            dma((groups, 2)),
            dma((groups, 2)),
            dma((shards,)),
            dma((shards,)),
        ],
        compiler_params=pltpu.CompilerParams(
            collective_id=0, has_side_effects=True, vmem_limit_bytes=24 * 2**20
        ),
        name="gather_project",
    )(*[
        pltpu.with_memory_space_constraint(a, pltpu.HBM)
        for a in (projectors, occupied, block, weights.reshape(1, n_occ), u_index, u_values)
    ])
    gathered, hub = [pltpu.with_memory_space_constraint(a, pltpu.VMEM) for a in (gathered, hub)]

    blocks = most_steps(part, BLOCKS)
    tile = part // blocks
    deep = min(DEEP, blocks)
    return pl.pallas_call(
        functools.partial(apply_kernel, folds, blocks),
        out_shape=jax.ShapeDtypeStruct((n_blk, columns), block.dtype),
        in_specs=[vector, vector],
        out_specs=anywhere,
        scratch_shapes=[
            pltpu.VMEM((deep, folds * n_blk, tile), block.dtype),
            dma((deep, folds)),
        ],
        compiler_params=pltpu.CompilerParams(vmem_limit_bytes=24 * 2**20),
        name="apply_potential",
    )(hub, gathered)


def solution(mesh):
    spread = P(("image", "band"), "ga")
    in_specs = (spread, spread, spread, P(("image", "band")), P(), P())
    return jax.shard_map(
        functools.partial(per_device, mesh.shape["band"], mesh.shape["ga"]),
        mesh=mesh, in_specs=in_specs, out_specs=spread, check_vma=False,
    )
```

```python
import functools
import math

import jax
import jax.numpy as jnp
from jax import lax
from jax.experimental import pallas as pl
from jax.experimental.pallas import tpu as pltpu
from jax.sharding import PartitionSpec as P

ORB = 5
LANES = 128
SUBLANES = 8
CORES = 2
STEPS = 10
SMALL = 8
BLOCKS = 5
PIECES = 16
DEEP = 2
MESH = pl.DeviceIdType.MESH
NT = (((1,), (1,)), ((), ()))


def most_steps(columns, limit):
    units = columns // LANES
    return max(s for s in range(1, limit + 1) if units % s == 0)


def round_up(n, to):
    return -(-n // to) * to


def plan(part):
    steps = most_steps(part, STEPS)
    width = part // steps
    units = width // LANES
    first = units // 8
    head = [first, units - first] if first and steps > 1 else [units]
    last, left = [], units
    while left > SMALL:
        last.append(left - left // 2)
        left //= 2
    last.append(left)
    sends = []
    for step, cuts in ((0, head),) * (steps > 1) + ((steps - 1, last),):
        at = step * width
        for cut in cuts:
            sends.append((step, at, cut * LANES))
            at += cut * LANES
    heads = [x for x in sends if x[0] == 0 and steps > 1]
    tails = [x for x in sends if x[0] == steps - 1]
    return steps, width, heads, tails


def gather_kernel(
    shards, groups, folds,
    p_ref, occ_ref, blk_ref, weights_hbm, index_hbm, table_hbm,
    all_ref, hub_ref,
    weights_ref, index_ref, table_ref, raw, bands, acc, proj, proj_all, diag, diag_all, select, scale, weight,
    small_sem, raw_sem, band_sem, chip_send, core_send, recv, ga_send, ga_recv, sum_send, sum_recv,
):
    chips = shards // CORES
    rows, columns = p_ref.shape
    part = columns // folds
    packed = rows * folds
    steps, width, heads, tails = plan(part)
    middle = max(steps - 2, 0)
    count = len(heads) + middle + len(tails)
    first_tail = len(heads) + middle
    n_occ, n_blk = occ_ref.shape[0], blk_ref.shape[0]
    both = n_occ + n_blk
    total = shards * rows
    wide = bands.shape[2]
    lanes = proj.shape[1]
    me = lax.axis_index("band")
    chip, core = me // CORES, lax.rem(me, CORES)
    ga = lax.axis_index("ga")
    partner = chip * CORES + (1 - core)

    def band_at(distance):
        return lax.rem(chip + distance, chips) * CORES + core

    def span(piece):
        if isinstance(piece, int) and piece < len(heads):
            return heads[piece][1:]
        if isinstance(piece, int) and piece >= first_tail:
            return tails[piece - first_tail][1:]
        return pl.multiple_of((piece - len(heads) + 1) * width, LANES), width

    def raw_copy(piece, fold):
        start, w = span(piece)
        return pltpu.make_async_copy(
            p_ref.at[:, pl.ds(fold * part + start, w)],
            raw.at[fold, :, pl.ds(start, w)],
            raw_sem.at[piece, fold],
        )

    def band_copies(step):
        slot = lax.rem(step, 2)
        found = []
        for fold in range(folds):
            cols = pl.ds(pl.multiple_of(fold * part + step * width, LANES), width)
            found.append(pltpu.make_async_copy(
                occ_ref.at[:, cols], bands.at[slot, fold, pl.ds(0, n_occ)], band_sem.at[slot, fold, 0]))
            found.append(pltpu.make_async_copy(
                blk_ref.at[:, cols], bands.at[slot, fold, pl.ds(n_occ, n_blk)], band_sem.at[slot, fold, 1]))
        return found

    def rows_of(step, owner):
        start, w = span(step)
        return all_ref.at[pl.ds(pl.multiple_of(owner * packed, SUBLANES), packed), pl.ds(start, w)]

    def to_chip(step, distance):
        slot = CORES * ((chips - distance) % chips)
        return pltpu.make_async_remote_copy(
            src_ref=rows_of(step, me), dst_ref=rows_of(step, me),
            send_sem=chip_send.at[step, distance], recv_sem=recv.at[step, slot],
            device_id={"band": band_at(distance)}, device_id_type=MESH)

    def to_core(step, distance):
        return pltpu.make_async_remote_copy(
            src_ref=rows_of(step, band_at(distance)), dst_ref=rows_of(step, band_at(distance)),
            send_sem=core_send.at[step, distance], recv_sem=recv.at[step, CORES * distance + 1],
            device_id={"band": partner}, device_id_type=MESH)

    def pack(step):
        start, w = span(step)
        for fold in range(folds):
            raw_copy(step, fold).wait()
        pieces = [raw[fold, :, pl.ds(start, w)].astype(jnp.float32) for fold in range(folds)]
        all_ref[pl.ds(pl.multiple_of(me * packed, SUBLANES), packed), pl.ds(start, w)] = (
            jnp.concatenate(pieces, axis=0).astype(all_ref.dtype))

    def send(step):
        for distance in range(1, chips):
            to_chip(step, distance).start()
        to_core(step, 0).start()

    for fold in range(folds):
        raw_copy(0, fold).start()
    barrier = pltpu.get_barrier_semaphore()
    for k in range(1, shards):
        pl.semaphore_signal(barrier, inc=1, device_id={"band": lax.rem(me + k, shards)}, device_id_type=MESH)
    for k in range(1, groups):
        pl.semaphore_signal(barrier, inc=1, device_id={"ga": lax.rem(ga + k, groups)}, device_id_type=MESH)
    pack(0)
    pl.semaphore_wait(barrier, shards + groups - 2)
    send(0)

    small = [
        pltpu.make_async_copy(source, target, small_sem.at[k])
        for k, (source, target) in enumerate(
            ((weights_hbm, weights_ref), (index_hbm, index_ref), (table_hbm, table_ref)))
    ]
    for copy in small:
        copy.start()

    def fetch(step):
        for fold in range(folds):
            raw_copy(step, fold).start()

    def loop(first, last, body):
        def run(step, carry):
            body(step)
            return carry
        lax.fori_loop(first, last, run, 0)

    def each(body, low):
        for piece in range(low, len(heads)):
            body(piece)
        loop(max(low, len(heads)), first_tail, body)
        for piece in range(max(low, first_tail), count):
            body(piece)

    each(fetch, 1)
    for step in range(min(2, steps)):
        for copy in band_copies(step):
            copy.start()

    def pack_send(piece):
        pack(piece)
        send(piece)

    each(pack_send, 1)
    acc[...] = jnp.zeros_like(acc)
    if wide > both:
        for slot in range(2):
            for fold in range(folds):
                bands[slot, fold, pl.ds(both, wide - both)] = jnp.zeros((wide - both, width), bands.dtype)
    shape = (lanes, shards * packed)
    row = lax.broadcasted_iota(jnp.int32, shape, 0)
    col = lax.broadcasted_iota(jnp.int32, shape, 1)
    for fold in range(folds):
        hits = jnp.zeros(shape, jnp.float32)
        for owner in range(shards):
            low = owner * packed + fold * rows
            hit = (col >= low) & (col < low + rows) & (col - row == low - owner * rows)
            hits = hits + jnp.where(hit, 1.0, 0.0)
        select[fold] = hits.astype(select.dtype)
    for copy in small:
        copy.wait()
    lane = lax.broadcasted_iota(jnp.int32, (SUBLANES, lanes), 1)
    values = jnp.zeros((SUBLANES, lanes), jnp.float32)
    orbital = jnp.zeros((SUBLANES, lanes), jnp.int32)
    for atom in range(total // ORB):
        inside = (lane >= atom * ORB) & (lane < (atom + 1) * ORB)
        values = jnp.where(inside, table_ref[index_ref[atom]], values)
        orbital = jnp.where(inside, lane - atom * ORB, orbital)
    scale[...] = values
    one = lax.broadcasted_iota(jnp.int32, (n_occ, n_occ), 0)
    two = lax.broadcasted_iota(jnp.int32, (n_occ, n_occ), 1)
    column = jnp.sum(jnp.where(one == two, jnp.broadcast_to(weights_ref[...], (n_occ, n_occ)), 0.0), axis=1, keepdims=True)
    weight[...] = jnp.broadcast_to(column, weight.shape)

    def forward(piece):
        for distance in range(1, chips):
            to_chip(piece, chips - distance).wait_recv()
            to_core(piece, distance).start()

    def project(piece, step, low):
        start, w = span(piece)
        slot = lax.rem(step, 2)
        for distance in range(chips):
            to_core(piece, distance).wait_recv()
        held = all_ref[:, pl.ds(start, w)]
        for fold in range(folds):
            acc[fold] += lax.dot_general(
                held, bands[slot, fold, :, pl.ds(low, w)], NT, preferred_element_type=jnp.float32)

    def sent(piece):
        for distance in range(1, chips):
            to_chip(piece, distance).wait_send()
        for distance in range(chips):
            to_core(piece, distance).wait_send()

    def landed(step):
        for copy in band_copies(step):
            copy.wait()

    def ahead(step):
        for copy in band_copies(step):
            copy.start()

    waiting = None
    for piece, (step, start, _) in enumerate(heads):
        forward(piece)
        if waiting is not None:
            project(*waiting)
        elif piece == 0:
            landed(0)
        waiting = (piece, 0, start)
    if middle:
        piece = len(heads)
        forward(piece)
        project(*waiting)
        for each_one in range(len(heads)):
            sent(each_one)
        ahead(2)

        def step_on(step):
            piece = step - 1 + len(heads)
            forward(piece)
            landed(step - 1)
            project(piece - 1, step - 1, 0)
            sent(piece - 1)
            ahead(step + 1)

        loop(2, steps - 1, step_on)
        waiting = (first_tail - 1, steps - 2, 0)
    for piece in range(first_tail, count):
        forward(piece)
        if piece == first_tail and middle:
            landed(steps - 2)
        if waiting is not None:
            project(*waiting)
        if piece == first_tail:
            landed(steps - 1)
        waiting = (piece, steps - 1, tails[piece - first_tail][1] - (steps - 1) * width)
    project(*waiting)

    pieces = []
    for owner in range(shards):
        piece = acc[0, pl.ds(owner * packed, rows)]
        for fold in range(1, folds):
            piece = piece + acc[fold, pl.ds(owner * packed + fold * rows, rows)]
        pieces.append(piece)
    if lanes > total:
        pieces.append(jnp.zeros((lanes - total, wide), jnp.float32))
    own = jnp.transpose(jnp.concatenate(pieces, axis=0))
    proj[...] = own

    def to_group(k, part_of):
        low, size = ((0, n_occ), (n_occ, n_blk))[part_of]
        return pltpu.make_async_remote_copy(
            src_ref=proj.at[pl.ds(low, size)], dst_ref=proj_all.at[k, pl.ds(low, size)],
            send_sem=ga_send.at[k, part_of], recv_sem=ga_recv.at[k, part_of],
            device_id={"ga": lax.rem(ga + k, groups)}, device_id_type=MESH)

    for part_of in range(2):
        for k in range(1, groups):
            to_group(k, part_of).start()
    for piece in range(max(first_tail - 1, 0) if middle else 0, count):
        sent(piece)
    mine = own[:n_occ]
    for k in range(1, groups):
        to_group(k, 0).wait_recv()
        mine = mine + proj_all[k, pl.ds(0, n_occ)]
    weighted = mine * weight[...]
    found = []
    for gap in range(ORB):
        moved = mine if gap == 0 else pltpu.roll(mine, lanes - gap, 1)
        found.append(jnp.sum(weighted * moved, axis=0, keepdims=True))
    found.append(jnp.zeros((SUBLANES - ORB, lanes), jnp.float32))
    occ = jnp.concatenate(found, axis=0)
    diag[...] = occ

    def to_band(k):
        return pltpu.make_async_remote_copy(
            src_ref=diag, dst_ref=diag_all.at[k], send_sem=sum_send.at[k], recv_sem=sum_recv.at[k],
            device_id={"band": lax.rem(me + k, shards)}, device_id_type=MESH)

    for k in range(1, shards):
        to_band(k).start()
    block = own[n_occ:both]
    for k in range(1, groups):
        to_group(k, 1).wait_recv()
        block = block + proj_all[k, pl.ds(n_occ, n_blk)]
    for k in range(1, shards):
        to_band(k).wait_recv()
        occ = occ + diag_all[k]
    u = scale[pl.ds(0, 1)]
    m = orbital[0:1]
    hub = (u * (0.5 - occ[0:1])) * block
    for gap in range(1, ORB):
        pair = -occ[gap:gap + 1]
        above = jnp.where(m + gap < ORB, u * pair, 0.0)
        below = jnp.where(m - gap >= 0, u * pltpu.roll(pair, gap, 1), 0.0)
        hub = hub + above * pltpu.roll(block, lanes - gap, 1) + below * pltpu.roll(block, gap, 1)
    hub = hub.astype(jnp.bfloat16)
    for fold in range(folds):
        hub_ref[pl.ds(fold * n_blk, n_blk)] = jnp.dot(
            hub, select[fold], preferred_element_type=jnp.float32).astype(jnp.bfloat16)

    for k in range(1, groups):
        for part_of in range(2):
            to_group(k, part_of).wait_send()
    for k in range(1, shards):
        to_band(k).wait_send()


def apply_kernel(folds, blocks, pieces, hub_ref, all_ref, out_ref, done, sems):
    bands = out_ref.shape[0]
    part = out_ref.shape[1] // folds
    tile = part // blocks
    size = tile // pieces
    deep = done.shape[0]

    def stores(step, piece):
        slot = lax.rem(step, deep)
        start = pl.multiple_of(step * tile, LANES) + piece * size
        return [pltpu.make_async_copy(
            done.at[slot, pl.ds(fold * bands, bands), pl.ds(piece * size, size)],
            out_ref.at[:, pl.ds(pl.multiple_of(fold * part + start, LANES), size)],
            sems.at[slot, piece, fold],
        ) for fold in range(folds)]

    def run(step, carry):
        @pl.when(step >= deep)
        def _():
            for piece in range(pieces):
                for copy in stores(step - deep, piece):
                    copy.wait()

        for piece in range(pieces):
            start = pl.multiple_of(step * tile + piece * size, LANES)
            done[lax.rem(step, deep), :, pl.ds(piece * size, size)] = jnp.dot(
                hub_ref[...], all_ref[:, pl.ds(start, size)],
                preferred_element_type=jnp.float32).astype(done.dtype)
            for copy in stores(step, piece):
                copy.start()
        return carry

    lax.fori_loop(0, blocks, run, 0)
    for step in range(max(blocks - deep, 0), blocks):
        for piece in range(pieces):
            for copy in stores(step, piece):
                copy.wait()


def per_device(shards, groups, projectors, occupied, block, weights, u_index, u_values):
    rows, columns = projectors.shape
    n_occ, n_blk = occupied.shape[0], block.shape[0]
    folds = SUBLANES // math.gcd(rows, SUBLANES)
    part = columns // folds
    steps, width, heads, tails = plan(part)
    count = len(heads) + max(steps - 2, 0) + len(tails)
    packed, total = rows * folds, rows * shards
    wide = round_up(n_occ + n_blk, LANES)
    lanes = round_up(total, LANES)
    anywhere = pl.BlockSpec(memory_space=pl.ANY)
    vector = pl.BlockSpec(memory_space=pltpu.VMEM)
    dma = pltpu.SemaphoreType.DMA
    chips = shards // CORES
    gathered, hub = pl.pallas_call(
        functools.partial(gather_kernel, shards, groups, folds),
        out_shape=(
            pltpu.VMEM((shards * packed, part), projectors.dtype),
            pltpu.VMEM((folds * n_blk, shards * packed), jnp.bfloat16),
        ),
        in_specs=[anywhere] * 6,
        out_specs=(vector, vector),
        scratch_shapes=[
            pltpu.VMEM((1, n_occ), jnp.float32),
            pltpu.SMEM(u_index.shape, u_index.dtype),
            pltpu.SMEM(u_values.shape, u_values.dtype),
            pltpu.VMEM((folds, rows, part), projectors.dtype),
            pltpu.VMEM((2, folds, wide, width), occupied.dtype),
            pltpu.VMEM((folds, shards * packed, wide), jnp.float32),
            pltpu.VMEM((wide, lanes), jnp.float32),
            pltpu.VMEM((groups, wide, lanes), jnp.float32),
            pltpu.VMEM((SUBLANES, lanes), jnp.float32),
            pltpu.VMEM((shards, SUBLANES, lanes), jnp.float32),
            pltpu.VMEM((folds, lanes, shards * packed), jnp.bfloat16),
            pltpu.VMEM((SUBLANES, lanes), jnp.float32),
            pltpu.VMEM((n_occ, lanes), jnp.float32),
            dma((3,)),
            dma((count, folds)),
            dma((2, folds, 2)),
            dma((count, chips)),
            dma((count, chips)),
            dma((count, shards)),
            dma((groups, 2)),
            dma((groups, 2)),
            dma((shards,)),
            dma((shards,)),
        ],
        compiler_params=pltpu.CompilerParams(
            collective_id=0, has_side_effects=True, vmem_limit_bytes=24 * 2**20
        ),
        name="gather_project",
    )(*[
        pltpu.with_memory_space_constraint(a, pltpu.HBM)
        for a in (projectors, occupied, block, weights.reshape(1, n_occ), u_index, u_values)
    ])
    gathered, hub = [pltpu.with_memory_space_constraint(a, pltpu.VMEM) for a in (gathered, hub)]

    blocks = most_steps(part, BLOCKS)
    tile = part // blocks
    pieces = most_steps(tile, PIECES)
    deep = min(DEEP, blocks)
    return pl.pallas_call(
        functools.partial(apply_kernel, folds, blocks, pieces),
        out_shape=jax.ShapeDtypeStruct((n_blk, columns), block.dtype),
        in_specs=[vector, vector],
        out_specs=anywhere,
        scratch_shapes=[
            pltpu.VMEM((deep, folds * n_blk, tile), block.dtype),
            dma((deep, pieces, folds)),
        ],
        compiler_params=pltpu.CompilerParams(vmem_limit_bytes=24 * 2**20),
        name="apply_potential",
    )(hub, gathered)


def solution(mesh):
    spread = P(("image", "band"), "ga")
    in_specs = (spread, spread, spread, P(("image", "band")), P(), P())
    return jax.shard_map(
        functools.partial(per_device, mesh.shape["band"], mesh.shape["ga"]),
        mesh=mesh, in_specs=in_specs, out_specs=spread, check_vma=False,
    )
```

```python
import functools
import math

import jax
import jax.numpy as jnp
from jax import lax
from jax.experimental import pallas as pl
from jax.experimental.pallas import tpu as pltpu
from jax.sharding import PartitionSpec as P

ORB = 5
LANES = 128
SUBLANES = 8
CORES = 2
STEPS = 10
SMALL = 8
BLOCKS = 5
PIECES = 8
DEEP = 2
MESH = pl.DeviceIdType.MESH
NT = (((1,), (1,)), ((), ()))


def most_steps(columns, limit):
    units = columns // LANES
    return max(s for s in range(1, limit + 1) if units % s == 0)


def round_up(n, to):
    return -(-n // to) * to


def plan(part):
    steps = most_steps(part, STEPS)
    width = part // steps
    units = width // LANES
    first = units // 8
    head = [first, units - first] if first and steps > 1 else [units]
    last, left = [], units
    while left > SMALL:
        last.append(left - left // 2)
        left //= 2
    last.append(left)
    sends = []
    for step, cuts in ((0, head),) * (steps > 1) + ((steps - 1, last),):
        at = step * width
        for cut in cuts:
            sends.append((step, at, cut * LANES))
            at += cut * LANES
    heads = [x for x in sends if x[0] == 0 and steps > 1]
    tails = [x for x in sends if x[0] == steps - 1]
    return steps, width, heads, tails


def gather_kernel(
    shards, groups, folds,
    p_ref, occ_ref, blk_ref, weights_hbm, index_hbm, table_hbm,
    all_ref, hub_ref,
    weights_ref, index_ref, table_ref, raw, bands, acc, proj, proj_all, diag, diag_all, select, scale, weight,
    small_sem, raw_sem, band_sem, chip_send, core_send, recv, ga_send, ga_recv, sum_send, sum_recv,
):
    chips = shards // CORES
    rows, columns = p_ref.shape
    part = columns // folds
    packed = rows * folds
    steps, width, heads, tails = plan(part)
    middle = max(steps - 2, 0)
    count = len(heads) + middle + len(tails)
    first_tail = len(heads) + middle
    n_occ, n_blk = occ_ref.shape[0], blk_ref.shape[0]
    both = n_occ + n_blk
    total = shards * rows
    wide = bands.shape[2]
    lanes = proj.shape[1]
    me = lax.axis_index("band")
    chip, core = me // CORES, lax.rem(me, CORES)
    ga = lax.axis_index("ga")
    partner = chip * CORES + (1 - core)

    def band_at(distance):
        return lax.rem(chip + distance, chips) * CORES + core

    def span(piece):
        if isinstance(piece, int) and piece < len(heads):
            return heads[piece][1:]
        if isinstance(piece, int) and piece >= first_tail:
            return tails[piece - first_tail][1:]
        return pl.multiple_of((piece - len(heads) + 1) * width, LANES), width

    def raw_copy(piece, fold):
        start, w = span(piece)
        return pltpu.make_async_copy(
            p_ref.at[:, pl.ds(fold * part + start, w)],
            raw.at[fold, :, pl.ds(start, w)],
            raw_sem.at[piece, fold],
        )

    def band_copies(step):
        slot = lax.rem(step, 2)
        found = []
        for fold in range(folds):
            cols = pl.ds(pl.multiple_of(fold * part + step * width, LANES), width)
            found.append(pltpu.make_async_copy(
                occ_ref.at[:, cols], bands.at[slot, fold, pl.ds(0, n_occ)], band_sem.at[slot, fold, 0]))
            found.append(pltpu.make_async_copy(
                blk_ref.at[:, cols], bands.at[slot, fold, pl.ds(n_occ, n_blk)], band_sem.at[slot, fold, 1]))
        return found

    def rows_of(step, owner):
        start, w = span(step)
        return all_ref.at[pl.ds(pl.multiple_of(owner * packed, SUBLANES), packed), pl.ds(start, w)]

    def to_chip(step, distance):
        slot = CORES * ((chips - distance) % chips)
        return pltpu.make_async_remote_copy(
            src_ref=rows_of(step, me), dst_ref=rows_of(step, me),
            send_sem=chip_send.at[step, distance], recv_sem=recv.at[step, slot],
            device_id={"band": band_at(distance)}, device_id_type=MESH)

    def to_core(step, distance):
        return pltpu.make_async_remote_copy(
            src_ref=rows_of(step, band_at(distance)), dst_ref=rows_of(step, band_at(distance)),
            send_sem=core_send.at[step, distance], recv_sem=recv.at[step, CORES * distance + 1],
            device_id={"band": partner}, device_id_type=MESH)

    def pack(step):
        start, w = span(step)
        for fold in range(folds):
            raw_copy(step, fold).wait()
        pieces = [raw[fold, :, pl.ds(start, w)].astype(jnp.float32) for fold in range(folds)]
        all_ref[pl.ds(pl.multiple_of(me * packed, SUBLANES), packed), pl.ds(start, w)] = (
            jnp.concatenate(pieces, axis=0).astype(all_ref.dtype))

    def send(step):
        for distance in range(1, chips):
            to_chip(step, distance).start()
        to_core(step, 0).start()

    for fold in range(folds):
        raw_copy(0, fold).start()
    barrier = pltpu.get_barrier_semaphore()
    for k in range(1, shards):
        pl.semaphore_signal(barrier, inc=1, device_id={"band": lax.rem(me + k, shards)}, device_id_type=MESH)
    for k in range(1, groups):
        pl.semaphore_signal(barrier, inc=1, device_id={"ga": lax.rem(ga + k, groups)}, device_id_type=MESH)
    pack(0)
    pl.semaphore_wait(barrier, shards + groups - 2)
    send(0)

    small = [
        pltpu.make_async_copy(source, target, small_sem.at[k])
        for k, (source, target) in enumerate(
            ((weights_hbm, weights_ref), (index_hbm, index_ref), (table_hbm, table_ref)))
    ]
    for copy in small:
        copy.start()

    def fetch(step):
        for fold in range(folds):
            raw_copy(step, fold).start()

    def loop(first, last, body):
        def run(step, carry):
            body(step)
            return carry
        lax.fori_loop(first, last, run, 0)

    def each(body, low):
        for piece in range(low, len(heads)):
            body(piece)
        loop(max(low, len(heads)), first_tail, body)
        for piece in range(max(low, first_tail), count):
            body(piece)

    each(fetch, 1)
    for step in range(min(2, steps)):
        for copy in band_copies(step):
            copy.start()

    def pack_send(piece):
        pack(piece)
        send(piece)

    each(pack_send, 1)
    acc[...] = jnp.zeros_like(acc)
    if wide > both:
        for slot in range(2):
            for fold in range(folds):
                bands[slot, fold, pl.ds(both, wide - both)] = jnp.zeros((wide - both, width), bands.dtype)
    shape = (lanes, shards * packed)
    row = lax.broadcasted_iota(jnp.int32, shape, 0)
    col = lax.broadcasted_iota(jnp.int32, shape, 1)
    for fold in range(folds):
        hits = jnp.zeros(shape, jnp.float32)
        for owner in range(shards):
            low = owner * packed + fold * rows
            hit = (col >= low) & (col < low + rows) & (col - row == low - owner * rows)
            hits = hits + jnp.where(hit, 1.0, 0.0)
        select[fold] = hits.astype(select.dtype)
    for copy in small:
        copy.wait()
    lane = lax.broadcasted_iota(jnp.int32, (SUBLANES, lanes), 1)
    values = jnp.zeros((SUBLANES, lanes), jnp.float32)
    orbital = jnp.zeros((SUBLANES, lanes), jnp.int32)
    for atom in range(total // ORB):
        inside = (lane >= atom * ORB) & (lane < (atom + 1) * ORB)
        values = jnp.where(inside, table_ref[index_ref[atom]], values)
        orbital = jnp.where(inside, lane - atom * ORB, orbital)
    scale[...] = values
    one = lax.broadcasted_iota(jnp.int32, (n_occ, n_occ), 0)
    two = lax.broadcasted_iota(jnp.int32, (n_occ, n_occ), 1)
    column = jnp.sum(jnp.where(one == two, jnp.broadcast_to(weights_ref[...], (n_occ, n_occ)), 0.0), axis=1, keepdims=True)
    weight[...] = jnp.broadcast_to(column, weight.shape)

    def forward(piece):
        for distance in range(1, chips):
            to_chip(piece, chips - distance).wait_recv()
            to_core(piece, distance).start()

    def project(piece, step, low):
        start, w = span(piece)
        slot = lax.rem(step, 2)
        for distance in range(chips):
            to_core(piece, distance).wait_recv()
        held = all_ref[:, pl.ds(start, w)]
        for fold in range(folds):
            acc[fold] += lax.dot_general(
                held, bands[slot, fold, :, pl.ds(low, w)], NT, preferred_element_type=jnp.float32)

    def sent(piece):
        for distance in range(1, chips):
            to_chip(piece, distance).wait_send()
        for distance in range(chips):
            to_core(piece, distance).wait_send()

    def landed(step):
        for copy in band_copies(step):
            copy.wait()

    def ahead(step):
        for copy in band_copies(step):
            copy.start()

    waiting = None
    for piece, (step, start, _) in enumerate(heads):
        forward(piece)
        if waiting is not None:
            project(*waiting)
        elif piece == 0:
            landed(0)
        waiting = (piece, 0, start)
    if middle:
        piece = len(heads)
        forward(piece)
        project(*waiting)
        for each_one in range(len(heads)):
            sent(each_one)
        ahead(2)

        def step_on(step):
            piece = step - 1 + len(heads)
            forward(piece)
            landed(step - 1)
            project(piece - 1, step - 1, 0)
            sent(piece - 1)
            ahead(step + 1)

        loop(2, steps - 1, step_on)
        waiting = (first_tail - 1, steps - 2, 0)
    for piece in range(first_tail, count):
        forward(piece)
        if piece == first_tail and middle:
            landed(steps - 2)
        if waiting is not None:
            project(*waiting)
        if piece == first_tail:
            landed(steps - 1)
        waiting = (piece, steps - 1, tails[piece - first_tail][1] - (steps - 1) * width)
    project(*waiting)

    pieces = []
    for owner in range(shards):
        piece = acc[0, pl.ds(owner * packed, rows)]
        for fold in range(1, folds):
            piece = piece + acc[fold, pl.ds(owner * packed + fold * rows, rows)]
        pieces.append(piece)
    if lanes > total:
        pieces.append(jnp.zeros((lanes - total, wide), jnp.float32))
    own = jnp.transpose(jnp.concatenate(pieces, axis=0))
    proj[...] = own

    def to_group(k, part_of):
        low, size = ((0, n_occ), (n_occ, n_blk))[part_of]
        return pltpu.make_async_remote_copy(
            src_ref=proj.at[pl.ds(low, size)], dst_ref=proj_all.at[k, pl.ds(low, size)],
            send_sem=ga_send.at[k, part_of], recv_sem=ga_recv.at[k, part_of],
            device_id={"ga": lax.rem(ga + k, groups)}, device_id_type=MESH)

    for part_of in range(2):
        for k in range(1, groups):
            to_group(k, part_of).start()
    for piece in range(max(first_tail - 1, 0) if middle else 0, count):
        sent(piece)
    mine = own[:n_occ]
    for k in range(1, groups):
        to_group(k, 0).wait_recv()
        mine = mine + proj_all[k, pl.ds(0, n_occ)]
    weighted = mine * weight[...]
    found = []
    for gap in range(ORB):
        moved = mine if gap == 0 else pltpu.roll(mine, lanes - gap, 1)
        found.append(jnp.sum(weighted * moved, axis=0, keepdims=True))
    found.append(jnp.zeros((SUBLANES - ORB, lanes), jnp.float32))
    occ = jnp.concatenate(found, axis=0)
    diag[...] = occ

    def to_band(k):
        return pltpu.make_async_remote_copy(
            src_ref=diag, dst_ref=diag_all.at[k], send_sem=sum_send.at[k], recv_sem=sum_recv.at[k],
            device_id={"band": lax.rem(me + k, shards)}, device_id_type=MESH)

    for k in range(1, shards):
        to_band(k).start()
    block = own[n_occ:both]
    for k in range(1, groups):
        to_group(k, 1).wait_recv()
        block = block + proj_all[k, pl.ds(n_occ, n_blk)]
    u = scale[pl.ds(0, 1)]
    m = orbital[0:1]
    terms = []
    for gap in range(1, ORB):
        terms.append((
            jnp.where(m + gap < ORB, u, 0.0), pltpu.roll(block, lanes - gap, 1),
            jnp.where(m - gap >= 0, u, 0.0), pltpu.roll(block, gap, 1)))
    for k in range(1, shards):
        to_band(k).wait_recv()
        occ = occ + diag_all[k]
    hub = (u * (0.5 - occ[0:1])) * block
    for gap, (u_above, above, u_below, below) in enumerate(terms, 1):
        pair = occ[gap:gap + 1]
        hub = hub - (u_above * pair) * above - (u_below * pltpu.roll(pair, gap, 1)) * below
    hub = hub.astype(jnp.bfloat16)
    for fold in range(folds):
        hub_ref[pl.ds(fold * n_blk, n_blk)] = jnp.dot(
            hub, select[fold], preferred_element_type=jnp.float32).astype(jnp.bfloat16)

    for k in range(1, groups):
        for part_of in range(2):
            to_group(k, part_of).wait_send()
    for k in range(1, shards):
        to_band(k).wait_send()


def apply_kernel(folds, blocks, pieces, hub_ref, all_ref, out_ref, done, sems):
    bands = out_ref.shape[0]
    part = out_ref.shape[1] // folds
    tile = part // blocks
    size = tile // pieces
    deep = done.shape[0]

    def stores(step, piece):
        slot = lax.rem(step, deep)
        start = pl.multiple_of(step * tile, LANES) + piece * size
        return [pltpu.make_async_copy(
            done.at[slot, pl.ds(fold * bands, bands), pl.ds(piece * size, size)],
            out_ref.at[:, pl.ds(pl.multiple_of(fold * part + start, LANES), size)],
            sems.at[slot, piece, fold],
        ) for fold in range(folds)]

    def run(step, carry):
        @pl.when(step >= deep)
        def _():
            for piece in range(pieces):
                for copy in stores(step - deep, piece):
                    copy.wait()

        for piece in range(pieces):
            start = pl.multiple_of(step * tile + piece * size, LANES)
            done[lax.rem(step, deep), :, pl.ds(piece * size, size)] = jnp.dot(
                hub_ref[...], all_ref[:, pl.ds(start, size)],
                preferred_element_type=jnp.float32).astype(done.dtype)
            for copy in stores(step, piece):
                copy.start()
        return carry

    lax.fori_loop(0, blocks, run, 0)
    for step in range(max(blocks - deep, 0), blocks):
        for piece in range(pieces):
            for copy in stores(step, piece):
                copy.wait()


def per_device(shards, groups, projectors, occupied, block, weights, u_index, u_values):
    rows, columns = projectors.shape
    n_occ, n_blk = occupied.shape[0], block.shape[0]
    folds = SUBLANES // math.gcd(rows, SUBLANES)
    part = columns // folds
    steps, width, heads, tails = plan(part)
    count = len(heads) + max(steps - 2, 0) + len(tails)
    packed, total = rows * folds, rows * shards
    wide = round_up(n_occ + n_blk, LANES)
    lanes = round_up(total, LANES)
    anywhere = pl.BlockSpec(memory_space=pl.ANY)
    vector = pl.BlockSpec(memory_space=pltpu.VMEM)
    dma = pltpu.SemaphoreType.DMA
    chips = shards // CORES
    gathered, hub = pl.pallas_call(
        functools.partial(gather_kernel, shards, groups, folds),
        out_shape=(
            pltpu.VMEM((shards * packed, part), projectors.dtype),
            pltpu.VMEM((folds * n_blk, shards * packed), jnp.bfloat16),
        ),
        in_specs=[anywhere] * 6,
        out_specs=(vector, vector),
        scratch_shapes=[
            pltpu.VMEM((1, n_occ), jnp.float32),
            pltpu.SMEM(u_index.shape, u_index.dtype),
            pltpu.SMEM(u_values.shape, u_values.dtype),
            pltpu.VMEM((folds, rows, part), projectors.dtype),
            pltpu.VMEM((2, folds, wide, width), occupied.dtype),
            pltpu.VMEM((folds, shards * packed, wide), jnp.float32),
            pltpu.VMEM((wide, lanes), jnp.float32),
            pltpu.VMEM((groups, wide, lanes), jnp.float32),
            pltpu.VMEM((SUBLANES, lanes), jnp.float32),
            pltpu.VMEM((shards, SUBLANES, lanes), jnp.float32),
            pltpu.VMEM((folds, lanes, shards * packed), jnp.bfloat16),
            pltpu.VMEM((SUBLANES, lanes), jnp.float32),
            pltpu.VMEM((n_occ, lanes), jnp.float32),
            dma((3,)),
            dma((count, folds)),
            dma((2, folds, 2)),
            dma((count, chips)),
            dma((count, chips)),
            dma((count, shards)),
            dma((groups, 2)),
            dma((groups, 2)),
            dma((shards,)),
            dma((shards,)),
        ],
        compiler_params=pltpu.CompilerParams(
            collective_id=0, has_side_effects=True, vmem_limit_bytes=24 * 2**20
        ),
        name="gather_project",
    )(*[
        pltpu.with_memory_space_constraint(a, pltpu.HBM)
        for a in (projectors, occupied, block, weights.reshape(1, n_occ), u_index, u_values)
    ])
    gathered, hub = [pltpu.with_memory_space_constraint(a, pltpu.VMEM) for a in (gathered, hub)]

    blocks = most_steps(part, BLOCKS)
    tile = part // blocks
    pieces = most_steps(tile, PIECES)
    deep = min(DEEP, blocks)
    return pl.pallas_call(
        functools.partial(apply_kernel, folds, blocks, pieces),
        out_shape=jax.ShapeDtypeStruct((n_blk, columns), block.dtype),
        in_specs=[vector, vector],
        out_specs=anywhere,
        scratch_shapes=[
            pltpu.VMEM((deep, folds * n_blk, tile), block.dtype),
            dma((deep, pieces, folds)),
        ],
        compiler_params=pltpu.CompilerParams(vmem_limit_bytes=24 * 2**20),
        name="apply_potential",
    )(hub, gathered)


def solution(mesh):
    spread = P(("image", "band"), "ga")
    in_specs = (spread, spread, spread, P(("image", "band")), P(), P())
    return jax.shard_map(
        functools.partial(per_device, mesh.shape["band"], mesh.shape["ga"]),
        mesh=mesh, in_specs=in_specs, out_specs=spread, check_vma=False,
    )
```
